32 devices in a mesh: cuts: 4 (over z), row: 8 (over y, x, core).
Axes of the slice: x: 2, y: 2, z: 4, core: 2. Of those that a mesh axis runs over, the one named last changes fastest.
Arguments:
- eigvecs: float32 [16384, 2048], P('row', 'cuts'), may hold values from -1.2 to 1.2
- slice_counts: int32 [4], P('cuts'), may hold values from 256 to 512, as said below
- occ_index: int32 [2048], P('cuts'), may hold values from 0 to 63
- occ_levels: float32 [64], replicated, may hold values from 0 to 1
Outputs:
- slab: float32 [4096, 16384], P('cuts', 'row')
The draws below stay inside these ranges and needn't reach their ends.
Inputs may be any that keep to these rules, and one draw needn't show every extreme that they name: `slice_counts`: some slice holds exactly 512 eigenvalues in every draw; the others at least half of that.
All inputs are finite; a program needn't handle non-finite values.
Results may differ from the reference program's by a relative error of at most 0.000062.
Values sent between devices are 32-bit elements; how exact they have to be, the bound alone decides.
No kernel may reach another device: no remote copies, remote signals or barrier semaphores. Data moves between devices by JAX's collectives and lax.ppermute only.
A program may use at most 128 MiB of HBM per device.

```python
import jax
import jax.numpy as jnp
from jax import lax

ORDER = 16384
BLOCK = 1024
SLAB_SUB = 256
EIG_DEV = 512
LEVELS = 64
EIGS = 2048
SLAB = 4096
N_CUTS = 4


def draw_slice_counts(key, part):
    first, second = jax.random.split(jax.random.fold_in(key, 11))
    counted = jax.random.randint(first, (N_CUTS,), EIG_DEV // 2, EIG_DEV + 1)
    full_one = jax.random.randint(second, (), 0, N_CUTS)
    return jnp.where(jnp.arange(N_CUTS) == full_one, EIG_DEV, counted).astype(jnp.int32)


def with_ends(array, stream_key, low, top_value):
    longest = array.shape.index(max(array.shape))
    spots = []
    for shift in (0, 1):
        where = [jax.random.randint(jax.random.fold_in(stream_key, axis), (), 0, length) for axis, length in enumerate(array.shape)]
        where[longest] = (where[longest] + shift) % array.shape[longest]
        spots.append(tuple(where))
    return array.at[spots[0]].set(low).at[spots[1]].set(top_value)


def block_levels(key, dims, pieces, low, largest):
    factor_of, own = 1.0, jax.random.fold_in(key, 6)
    for position, shards_of in pieces:
        draws = jnp.exp(jax.random.uniform(jax.random.fold_in(own, position), (shards_of,), jnp.float32, low / len(pieces), largest / len(pieces)))
        factor_of = factor_of * jnp.repeat(draws, dims[position] // shards_of).reshape([-1 if axis == position else 1 for axis in range(len(dims))])
    return factor_of


def gaussian(own_key, shape, width, reach, pieces=(), held_as=jnp.bfloat16):
    array = jax.random.normal(own_key, shape, jnp.float32) * width
    if len(pieces) > 0:
        array = block_levels(own_key, shape, pieces, -0.22, 0.18) * array
    return jnp.clip(array, min=-reach, max=reach).astype(held_as)


def setup_inputs(seed: int = 0) -> dict:
    key_of = jax.random.split(jax.random.key(seed), 5)
    eigvecs = gaussian(key_of[0], (ORDER, EIGS), 0.18, 1.2, ((0, 8), (1, 4)), jnp.float32)
    slice_counts = draw_slice_counts(jax.random.fold_in(key_of[4], 71), 0)
    occ_index = with_ends(jax.random.randint(key_of[2], (EIGS,), 0, LEVELS), jax.random.fold_in(key_of[2], 1), 0, LEVELS - 1).astype(jnp.int32)
    occ_levels = jnp.clip(jax.random.uniform(key_of[3], (LEVELS,), jnp.float32, 0.0, 1.0), 0.0, 1.0)
    return dict(eigvecs=eigvecs, slice_counts=slice_counts, occ_index=occ_index, occ_levels=occ_levels)


def reference(eigvecs, slice_counts, occ_index, occ_levels):
    slots = jnp.arange(EIGS, dtype=jnp.int32)
    group = slots // EIG_DEV
    inside = slots - group * EIG_DEV
    live = inside < slice_counts[group]
    weights = jnp.where(live, occ_levels[occ_index], jnp.float32(0.0))
    blocks = eigvecs.reshape(ORDER // BLOCK, BLOCK, EIGS)[:, :SLAB_SUB, :]
    picked = blocks.reshape(SLAB, EIGS) * weights[None, :]
    return lax.dot_general(picked, eigvecs, (((1,), (1,)), ((), ())), precision=lax.Precision.HIGHEST, preferred_element_type=jnp.float32)
```

```python
import functools

import jax
import jax.numpy as jnp
from jax import lax
from jax.experimental import pallas as pl
from jax.experimental.pallas import tpu as pltpu
from jax.sharding import PartitionSpec as P


BLOCK = 1024
SLAB_SUB = 256
TILE = 256
SIZES = (2, 1, 1, 1, 1)
STRIDE = 32
PIECES = 8


def slot_weights(slice_counts, occ_index, occ_levels):
    level_ids = jnp.arange(occ_levels.shape[0], dtype=jnp.int32)
    one_hot = (occ_index[:, None] == level_ids[None, :]).astype(jnp.float32)
    values = jnp.dot(one_hot, occ_levels, precision=lax.Precision.HIGHEST)
    live = jnp.arange(occ_index.shape[0], dtype=jnp.int32) < slice_counts[0]
    return jnp.where(live, values, jnp.float32(0.0))


def split(value):
    high = value.astype(jnp.bfloat16)
    return high, (value - high.astype(jnp.float32)).astype(jnp.bfloat16)


def product_kernel(shape, always, with_base, tiles, flag, rows_ref, *refs):
    parts = []
    for counts in shape:
        parts.append([])
        for count in counts:
            parts[-1].append(refs[:count])
            refs = refs[count:]
    out_ref, rows_f32, a_both, b_both, arrived = refs[int(with_base) :]
    step = pl.program_id(0)
    depth = parts[0][0][0].shape[1]
    pieces, height = rows_f32.shape[0], rows_f32.shape[1]

    def copy(i):
        at = pl.ds(pl.multiple_of(i * height, height), height)
        return pltpu.make_async_copy(rows_ref.at[at, :], rows_f32.at[i], arrived.at[i])

    def multiply():
        @pl.when(step == 0)
        def _():
            @pl.loop(0, pieces)
            def _(i):
                copy(i).start()

        for index, tile_parts in enumerate(parts):

            @pl.when(step == index)
            def _():
                for q, terms in enumerate(tile_parts):
                    at = slice(q * depth, (q + 1) * depth)

                    @pl.loop(0, TILE // STRIDE)
                    def _(j):
                        rows = pl.ds(pl.multiple_of(j * STRIDE, STRIDE), STRIDE)
                        value = functools.reduce(jnp.add, [term[rows, :] for term in terms])
                        b_both[0, rows, at], b_both[1, rows, at] = split(value)

        @pl.when(step == 0)
        def _():
            @pl.loop(0, pieces)
            def _(i):
                copy(i).wait()

                @pl.loop(0, height // STRIDE)
                def _(j):
                    at = pl.ds(pl.multiple_of(j * STRIDE, STRIDE), STRIDE)
                    to = pl.ds(pl.multiple_of(i * height + j * STRIDE, STRIDE), STRIDE)
                    a_both[0, to, :], a_both[1, to, :] = split(rows_f32[i, at, :])

        dims = (((1,), (1,)), ((), ()))
        dot = functools.partial(
            lax.dot_general, dimension_numbers=dims, preferred_element_type=jnp.float32
        )
        out_ref[...] = dot(a_both[0], b_both[0])

        @pl.loop(1, 3)
        def _(term):
            out_ref[...] += dot(a_both[term % 2], b_both[term // 2])

    if always:
        multiply()
    else:
        pl.when(flag[0] == 0)(multiply)


def product(rows, parts, flag, tiles, all_columns, always=False, base=None):
    owned, depth = rows.shape
    slots = parts[0][0][0][0].shape[1]
    shape = [[len(terms) for terms in tile_parts] for tile_parts in parts]
    operands = [rows]
    in_specs = [pl.BlockSpec(memory_space=pl.ANY)]
    for tile_parts in parts:
        for terms in tile_parts:
            for array, block in terms:
                operands.append(array)
                in_specs.append(
                    pl.BlockSpec(
                        (TILE, slots),
                        lambda i, t, f, block=block: (block, 0),
                        pipeline_mode=pl.Buffered(1),
                    )
                )
    aliases = {}
    if base is not None:
        aliases = {2 + len(operands): 0}
        in_specs.append(pl.BlockSpec(memory_space=pl.ANY))
        operands.append(base)
    return pl.pallas_call(
        functools.partial(product_kernel, shape, always, base is not None),
        grid_spec=pltpu.PrefetchScalarGridSpec(
            num_scalar_prefetch=2,
            grid=(len(tiles),),
            in_specs=in_specs,
            out_specs=pl.BlockSpec((owned, TILE), lambda i, t, f: (0, t[i])),
            scratch_shapes=[
                pltpu.VMEM((PIECES, owned // PIECES, depth), jnp.float32),
                pltpu.VMEM((2, owned, depth), jnp.bfloat16),
                pltpu.VMEM((2, TILE, depth), jnp.bfloat16),
                pltpu.SemaphoreType.DMA((PIECES,)),
            ],
        ),
        out_shape=jax.ShapeDtypeStruct((owned, all_columns), jnp.float32),
        input_output_aliases=aliases,
        cost_estimate=pl.CostEstimate(
            flops=6 * owned * TILE * len(tiles) * depth,
            bytes_accessed=4 * (owned * depth + TILE * len(tiles) * (depth + owned)),
            transcendentals=0,
        ),
        name="product",
    )(jnp.asarray(tiles, jnp.int32), flag, *operands)


def place_kernel(tiles, flag, base_ref, sent_ref, out_ref, held, done):
    @pl.when(flag[0] != 0)
    def _():
        for index, tile in enumerate(tiles):
            take = pltpu.make_async_copy(
                sent_ref.at[:, pl.ds(index * TILE, TILE)], held.at[index], done.at[index]
            )
            take.start()
        for index, tile in enumerate(tiles):
            pltpu.make_async_copy(
                sent_ref.at[:, pl.ds(index * TILE, TILE)], held.at[index], done.at[index]
            ).wait()
            pltpu.make_async_copy(
                held.at[index], out_ref.at[:, pl.ds(tile * TILE, TILE)], done.at[index]
            ).start()
        for index, tile in enumerate(tiles):
            pltpu.make_async_copy(
                held.at[index], out_ref.at[:, pl.ds(tile * TILE, TILE)], done.at[index]
            ).wait()


def place(base, sent, flag, tiles):
    owned = base.shape[0]
    hbm = pl.BlockSpec(memory_space=pl.ANY)
    return pl.pallas_call(
        functools.partial(place_kernel, tiles),
        in_specs=[pl.BlockSpec(memory_space=pltpu.SMEM), hbm, hbm],
        out_specs=hbm,
        scratch_shapes=[
            pltpu.VMEM((len(tiles), owned, TILE), jnp.float32),
            pltpu.SemaphoreType.DMA((len(tiles),)),
        ],
        out_shape=jax.ShapeDtypeStruct(base.shape, base.dtype),
        input_output_aliases={1: 0},
        cost_estimate=pl.CostEstimate(
            flops=0, bytes_accessed=8 * owned * TILE * len(tiles), transcendentals=0
        ),
        name="place",
    )(flag, base, sent)


def slab_block(eigvecs, slice_counts, occ_index, occ_levels):
    row_count, slot_count = eigvecs.shape
    cuts = lax.axis_size("cuts")
    row_devices = lax.axis_size("row")
    cut = lax.axis_index("cuts")
    last = cuts - 1
    turns = [0, 1, last] + list(range(2, last))
    at_end = ((cut == 0) | (cut == last)).astype(jnp.int32).reshape(1)

    weights = slot_weights(slice_counts, occ_index, occ_levels)
    blocks = eigvecs.reshape(row_count // BLOCK, BLOCK, slot_count)
    picked = blocks[:, :SLAB_SUB, :].reshape(-1, slot_count)
    halves = row_devices // cuts

    up, down = [picked], [picked]
    for step in range(1, cuts):
        up.append(lax.ppermute(up[-1], "cuts", [(i, i + 1) for i in range(step - 1, last)]))
        down.append(lax.ppermute(down[-1], "cuts", [(i + 1, i) for i in range(last - step + 1)]))
    every = [(picked,)] + [(up[turn], down[cuts - turn]) for turn in turns[1:]]

    def spread(rows):
        return lax.all_to_all(rows, "row", split_axis=0, concat_axis=0, tiled=True)

    def to_plane(strips, block):
        strip = strips.shape[0] // cuts
        return lax.dynamic_slice_in_dim(strips, block * strip, strip, axis=0)

    def gathered(wide):
        wide = wide.reshape(halves, wide.shape[0] // halves, wide.shape[1])
        wide = lax.all_gather(wide, "row", axis=1, tiled=True)
        return wide.reshape(-1, wide.shape[2])

    def end_of(plane):
        return jnp.where(plane == 1, 0, last)

    strips = spread(picked * weights[None, :])
    other, own = [to_plane(strips, end_of(cut))], [to_plane(strips, cut)]
    for turn in turns[1:]:
        pairs = [(i, (i + turn) % cuts) for i in range(cuts)]
        inner = [(i, j) for i, j in pairs if j in (1, last - 1)]
        piece = to_plane(strips, end_of((cut + turn) % cuts))
        other.append(lax.ppermute(piece, "cuts", inner))
        piece = to_plane(strips, (cut + turn) % cuts)
        own.append(lax.ppermute(piece, "cuts", pairs))
    other = gathered(jnp.concatenate(other, axis=1))
    own = gathered(jnp.concatenate(own, axis=1))

    groups, tile_parts = unpicked_groups(row_count), {}
    for group in groups:
        mine = jnp.concatenate([eigvecs[t * TILE : (t + 1) * TILE] for t in group], axis=0)
        parts = [mine]
        for turn in turns[1:]:
            pairs = [(i, (i + turn) % cuts) for i in range(cuts)]
            pairs = [(i, j) for i, j in pairs if 0 < j < last]
            parts.append(lax.ppermute(mine, "cuts", pairs))
        for block, tile in enumerate(group):
            tile_parts[tile] = [[(part, block)] for part in parts]
    sents = {}
    for tile, parts in tile_parts.items():
        served = product(other, [parts], at_end, [0], TILE)
        sents[tile] = lax.ppermute(served, "cuts", [(1, 0), (last - 1, last)])

    picked_tiles = [t for t in range(row_count // TILE) if (t * TILE) % BLOCK < SLAB_SUB]
    picked_parts = [
        [[(term, block) for term in terms] for terms in every] for block in range(len(picked_tiles))
    ]
    out = product(own, picked_parts, at_end, picked_tiles, row_count, always=True)
    for group in owned_groups(row_count):
        out = product(own, [tile_parts[t] for t in group], at_end, group, row_count, base=out)
    for tile, sent in sents.items():
        out = place(out, sent, at_end, [tile])
    return out


def unpicked_groups(row_count):
    tiles = [t for t in range(row_count // TILE) if (t * TILE) % BLOCK >= SLAB_SUB]
    groups = []
    for size in SIZES:
        groups.append(tiles[:size])
        tiles = tiles[size:]
    return [g for g in groups + [tiles] if g]


def owned_groups(row_count):
    tiles = [t for group in unpicked_groups(row_count) for t in group]
    return [tiles[i : i + 2] for i in range(0, len(tiles), 2)]


def solution(mesh):
    return jax.shard_map(
        slab_block,
        mesh=mesh,
        in_specs=(P("row", "cuts"), P("cuts"), P("cuts"), P()),
        out_specs=P("cuts", "row"),
        check_vma=False,
    )
```

```python
import functools

import jax
import jax.numpy as jnp
from jax import lax
from jax.experimental import pallas as pl
from jax.experimental.pallas import tpu as pltpu
from jax.sharding import PartitionSpec as P


BLOCK = 1024
SLAB_SUB = 256
TILE = 256
OWNED = 2
SIZES = (1, 1, 1, 1, 1, 1)
STRIDE = 32
STEP = 64
PIECES = 8


def slot_weights(slice_counts, occ_index, occ_levels):
    level_ids = jnp.arange(occ_levels.shape[0], dtype=jnp.int32)
    one_hot = (occ_index[:, None] == level_ids[None, :]).astype(jnp.float32)
    values = jnp.dot(one_hot, occ_levels, precision=lax.Precision.HIGHEST)
    live = jnp.arange(occ_index.shape[0], dtype=jnp.int32) < slice_counts[0]
    return jnp.where(live, values, jnp.float32(0.0))


def split(value):
    high = value.astype(jnp.bfloat16)
    return high, (value - high.astype(jnp.float32)).astype(jnp.bfloat16)


def product_kernel(shape, always, with_base, tiles, flag, rows_ref, *refs):
    parts = []
    for counts in shape:
        parts.append([])
        for count in counts:
            parts[-1].append(refs[:count])
            refs = refs[count:]
    out_ref, rows_f32, a_both, b_both, arrived = refs[int(with_base) :]
    step = pl.program_id(0)
    depth = parts[0][0][0].shape[1]
    pieces, height = rows_f32.shape[0], rows_f32.shape[1]

    def copy(i):
        at = pl.ds(pl.multiple_of(i * height, height), height)
        return pltpu.make_async_copy(rows_ref.at[at, :], rows_f32.at[i], arrived.at[i])

    def multiply():
        @pl.when(step == 0)
        def _():
            @pl.loop(0, pieces)
            def _(i):
                copy(i).start()

        for index, tile_parts in enumerate(parts):

            @pl.when(step == index if len(parts) > 1 else step >= 0)
            def _():
                for q, terms in enumerate(tile_parts):
                    at = slice(q * depth, (q + 1) * depth)

                    @pl.loop(0, TILE // STEP)
                    def _(j):
                        rows = pl.ds(pl.multiple_of(j * STEP, STEP), STEP)
                        value = functools.reduce(jnp.add, [term[rows, :] for term in terms])
                        b_both[0, rows, at], b_both[1, rows, at] = split(value)

        @pl.when(step == 0)
        def _():
            @pl.loop(0, pieces)
            def _(i):
                copy(i).wait()

                @pl.loop(0, height // STRIDE)
                def _(j):
                    at = pl.ds(pl.multiple_of(j * STRIDE, STRIDE), STRIDE)
                    to = pl.ds(pl.multiple_of(i * height + j * STRIDE, STRIDE), STRIDE)
                    a_both[0, to, :], a_both[1, to, :] = split(rows_f32[i, at, :])

        dims = (((1,), (1,)), ((), ()))
        dot = functools.partial(
            lax.dot_general, dimension_numbers=dims, preferred_element_type=jnp.float32
        )
        out_ref[...] = (
            dot(a_both[0], b_both[0]) + dot(a_both[1], b_both[0]) + dot(a_both[0], b_both[1])
        )

    if always:
        multiply()
    else:
        pl.when(flag[0] == 0)(multiply)


def product(rows, parts, flag, tiles, all_columns, always=False, base=None):
    owned, depth = rows.shape
    slots = parts[0][0][0][0].shape[1]
    same = all(
        array is first and block == index
        for index, tile_parts in enumerate(parts)
        for terms, first_terms in zip(tile_parts, parts[0])
        for (array, block), (first, _) in zip(terms, first_terms)
    )
    shown = parts[:1] if same else parts
    shape = [[len(terms) for terms in tile_parts] for tile_parts in shown]
    operands = [rows]
    in_specs = [pl.BlockSpec(memory_space=pl.ANY)]
    for tile_parts in shown:
        for terms in tile_parts:
            for array, block in terms:
                operands.append(array)
                if same:
                    spec = pl.BlockSpec((TILE, slots), lambda i, t, f: (i, 0))
                else:
                    spec = pl.BlockSpec(
                        (TILE, slots),
                        lambda i, t, f, block=block: (block, 0),
                        pipeline_mode=pl.Buffered(1),
                    )
                in_specs.append(spec)
    aliases = {}
    if base is not None:
        aliases = {2 + len(operands): 0}
        in_specs.append(pl.BlockSpec(memory_space=pl.ANY))
        operands.append(base)
    return pl.pallas_call(
        functools.partial(product_kernel, shape, always, base is not None),
        grid_spec=pltpu.PrefetchScalarGridSpec(
            num_scalar_prefetch=2,
            grid=(len(tiles),),
            in_specs=in_specs,
            out_specs=pl.BlockSpec((owned, TILE), lambda i, t, f: (0, t[i])),
            scratch_shapes=[
                pltpu.VMEM((PIECES, owned // PIECES, depth), jnp.float32),
                pltpu.VMEM((2, owned, depth), jnp.bfloat16),
                pltpu.VMEM((2, TILE, depth), jnp.bfloat16),
                pltpu.SemaphoreType.DMA((PIECES,)),
            ],
        ),
        out_shape=jax.ShapeDtypeStruct((owned, all_columns), jnp.float32),
        input_output_aliases=aliases,
        cost_estimate=pl.CostEstimate(
            flops=6 * owned * TILE * len(tiles) * depth,
            bytes_accessed=4 * (owned * depth + TILE * len(tiles) * (depth + owned)),
            transcendentals=0,
        ),
        name="product",
    )(jnp.asarray(tiles, jnp.int32), flag, *operands)


def place_kernel(tiles, flag, base_ref, sent_ref, out_ref, held, done):
    @pl.when(flag[0] != 0)
    def _():
        for index, tile in enumerate(tiles):
            take = pltpu.make_async_copy(
                sent_ref.at[:, pl.ds(index * TILE, TILE)], held.at[index], done.at[index]
            )
            take.start()
        for index, tile in enumerate(tiles):
            pltpu.make_async_copy(
                sent_ref.at[:, pl.ds(index * TILE, TILE)], held.at[index], done.at[index]
            ).wait()
            pltpu.make_async_copy(
                held.at[index], out_ref.at[:, pl.ds(tile * TILE, TILE)], done.at[index]
            ).start()
        for index, tile in enumerate(tiles):
            pltpu.make_async_copy(
                held.at[index], out_ref.at[:, pl.ds(tile * TILE, TILE)], done.at[index]
            ).wait()


def place(base, sent, flag, tiles):
    owned = base.shape[0]
    hbm = pl.BlockSpec(memory_space=pl.ANY)
    return pl.pallas_call(
        functools.partial(place_kernel, tiles),
        in_specs=[pl.BlockSpec(memory_space=pltpu.SMEM), hbm, hbm],
        out_specs=hbm,
        scratch_shapes=[
            pltpu.VMEM((len(tiles), owned, TILE), jnp.float32),
            pltpu.SemaphoreType.DMA((len(tiles),)),
        ],
        out_shape=jax.ShapeDtypeStruct(base.shape, base.dtype),
        input_output_aliases={1: 0},
        cost_estimate=pl.CostEstimate(
            flops=0, bytes_accessed=8 * owned * TILE * len(tiles), transcendentals=0
        ),
        name="place",
    )(flag, base, sent)


def slab_block(eigvecs, slice_counts, occ_index, occ_levels):
    row_count, slot_count = eigvecs.shape
    cuts = lax.axis_size("cuts")
    row_devices = lax.axis_size("row")
    cut = lax.axis_index("cuts")
    last = cuts - 1
    turns = [0, 1, 3, 2] if cuts == 4 else list(range(cuts))
    at_end = ((cut == 0) | (cut == last)).astype(jnp.int32).reshape(1)

    weights = slot_weights(slice_counts, occ_index, occ_levels)
    blocks = eigvecs.reshape(row_count // BLOCK, BLOCK, slot_count)
    picked = blocks[:, :SLAB_SUB, :].reshape(-1, slot_count)
    halves = row_devices // cuts

    def moved(array, pairs):
        return lax.ppermute(array, "cuts", pairs)

    swap, outward = [(1, 2), (2, 1)], [(1, 0), (2, 3)]
    if cuts == 4:
        beside = moved(picked, [(i, i ^ 1) for i in range(cuts)])
        across = moved(picked, swap)
        onward = moved(beside, swap)
        every = [
            (picked,), (beside,), (across, moved(onward, outward)), (onward, moved(across, outward))
        ]
    else:
        every = [(picked,)]
        for turn in turns[1:]:
            every.append((moved(picked, [(i, i ^ turn) for i in range(cuts)]),))

    def spread(rows):
        return lax.all_to_all(rows, "row", split_axis=0, concat_axis=0, tiled=True)

    def to_plane(strips, block):
        strip = strips.shape[0] // cuts
        return lax.dynamic_slice_in_dim(strips, block * strip, strip, axis=0)

    def gathered(wide):
        wide = wide.reshape(halves, wide.shape[0] // halves, wide.shape[1])
        wide = lax.all_gather(wide, "row", axis=1, tiled=True)
        return wide.reshape(-1, wide.shape[2])

    def end_of(plane):
        return jnp.where(plane == 1, 0, last)

    strips = spread(picked * weights[None, :])
    other, own = [to_plane(strips, end_of(cut))], [to_plane(strips, cut)]
    for turn in turns[1:]:
        pairs = [(i, i ^ turn) for i in range(cuts)]
        inner = [(i, j) for i, j in pairs if j in (1, last - 1)]
        other.append(moved(to_plane(strips, end_of(cut ^ turn)), inner))
        own.append(moved(to_plane(strips, cut ^ turn), pairs))
    other = gathered(jnp.concatenate(other, axis=1))
    own = gathered(jnp.concatenate(own, axis=1))

    groups, tile_parts = unpicked_groups(row_count), {}
    for group in groups:
        mine = jnp.concatenate([eigvecs[t * TILE : (t + 1) * TILE] for t in group], axis=0)
        if cuts == 4:
            beside = moved(mine, [(0, 1), (3, 2)])
            across = moved(mine, swap)
            parts = [mine, beside, across, moved(beside, swap)]
        else:
            parts = [mine]
            for turn in turns[1:]:
                pairs = [(i, i ^ turn) for i in range(cuts)]
                pairs = [(i, j) for i, j in pairs if 0 < j < last]
                parts.append(moved(mine, pairs))
        for block, tile in enumerate(group):
            tile_parts[tile] = [[(part, block)] for part in parts]
    sents = {}
    for tile, parts in tile_parts.items():
        served = product(other, [parts], at_end, [0], TILE)
        sents[tile] = lax.ppermute(served, "cuts", [(1, 0), (last - 1, last)])

    picked_tiles = [t for t in range(row_count // TILE) if (t * TILE) % BLOCK < SLAB_SUB]
    picked_parts = [
        [[(term, block) for term in terms] for terms in every] for block in range(len(picked_tiles))
    ]
    out = product(own, picked_parts, at_end, picked_tiles, row_count, always=True)
    for group in owned_groups(row_count):
        out = product(own, [tile_parts[t] for t in group], at_end, group, row_count, base=out)
    for tile, sent in sents.items():
        out = place(out, sent, at_end, [tile])
    return out


def unpicked_groups(row_count):
    tiles = [t for t in range(row_count // TILE) if (t * TILE) % BLOCK >= SLAB_SUB]
    groups = []
    for size in SIZES:
        groups.append(tiles[:size])
        tiles = tiles[size:]
    return [g for g in groups + [tiles] if g]


def owned_groups(row_count):
    tiles = [t for group in unpicked_groups(row_count) for t in group]
    return [g for g in (tiles[:OWNED], tiles[OWNED:]) if g]


def solution(mesh):
    return jax.shard_map(
        slab_block,
        mesh=mesh,
        in_specs=(P("row", "cuts"), P("cuts"), P("cuts"), P()),
        out_specs=P("cuts", "row"),
        check_vma=False,
    )
```
